16 devices in a mesh: dp: 4 (over y, z), tp: 4 (over x, core).
Axes of the slice: x: 2, y: 2, z: 2, core: 2. Of those that a mesh axis runs over, the one named last changes fastest.
Arguments:
- x: bfloat16 [4, 2048, 2048], P('dp', 'tp')
- dy: bfloat16 [4, 2048, 2048], P('dp', 'tp')
- wq: bfloat16 [2048, 2048], P('dp', 'tp')
- wk: bfloat16 [2048, 512], P('dp', 'tp')
- wv: bfloat16 [2048, 512], P('dp', 'tp')
- wo: bfloat16 [2048, 2048], P(('tp', 'dp'))
- w_gate: bfloat16 [2048, 7168], P('dp', 'tp')
- w_up: bfloat16 [2048, 7168], P('dp', 'tp')
- w_down: bfloat16 [7168, 2048], P(('tp', 'dp'))
Outputs:
- output 1: bfloat16 [4, 2048, 2048], P('dp', 'tp')
- output 2: bfloat16 [2048, 2048], P('dp', 'tp')
- output 3: bfloat16 [2048, 512], P('dp', 'tp')
- output 4: bfloat16 [2048, 512], P('dp', 'tp')
- output 5: bfloat16 [2048, 2048], P(('tp', 'dp'))
- output 6: bfloat16 [2048, 7168], P('dp', 'tp')
- output 7: bfloat16 [2048, 7168], P('dp', 'tp')
- output 8: bfloat16 [7168, 2048], P(('tp', 'dp'))
All inputs are finite; a program needn't handle non-finite values.
Results may differ from the reference program's by a relative error of at most 0.024.
Values are sent between devices in bfloat16 or wider.
A program may use at most 2 GiB of HBM per device.

```python
import jax
import jax.numpy as jnp
from jax import lax

SEQUENCES = 4
TOKENS = 2048
D = 2048
HEADS = 16
KV_HEADS = 4
HEAD = 128
FF = 7168
THETA = 10000
NAMES = ("wq", "wk", "wv", "wo", "w_gate", "w_up", "w_down")
SHAPES = {
    "wq": (D, HEADS * HEAD),
    "wk": (D, KV_HEADS * HEAD),
    "wv": (D, KV_HEADS * HEAD),
    "wo": (HEADS * HEAD, D),
    "w_gate": (D, FF),
    "w_up": (D, FF),
    "w_down": (FF, D),
}


def bump(key, n, height):
    away = (jnp.arange(n, dtype=jnp.int32) - jax.random.randint(key, (), 0, n, jnp.int32)) % n
    return jnp.where(away < n // 8, height, 1.0)


def together(key, own, strength):
    shared = jax.random.normal(key, own.shape[1:], jnp.float32)
    return (own + strength * shared) * lax.rsqrt(1 + strength * strength)


def setup_inputs(seed: int = 0, part: int = 0) -> dict:
    kx, kdy, ka, kb, kz, kf, kh, kl, *kw = jax.random.split(jax.random.key(seed), 8 + len(NAMES))
    shape = (SEQUENCES, TOKENS, D)
    much_x, much_dy = jax.random.uniform(kz, (2,), jnp.float32, 0.0, 1.0)
    loud = 2.0 ** jax.random.uniform(jax.random.fold_in(kz, 1), (), jnp.float32, -1.0, 2.0)
    halves = 2.0 ** jax.random.uniform(kl, (2,), jnp.float32, -1.0, 1.0)
    times = {"wq": 1.0, "wk": 1.0, "wv": 2.0, "wo": halves[0], "w_gate": 1.0, "w_up": bump(kh, FF, 4.0), "w_down": halves[1]}
    x = together(ka, jax.random.normal(kx, shape, jnp.float32), much_x) * bump(kf, D, 4.0)
    dy = together(kb, jax.random.normal(kdy, shape, jnp.float32), much_dy)
    drawn = {"x": x.astype(jnp.bfloat16), "dy": (loud * dy * (SEQUENCES * TOKENS) ** -0.5).astype(jnp.bfloat16)}
    for key, name in zip(kw, NAMES, strict=True):
        drawn[name] = (jax.random.normal(key, SHAPES[name], jnp.float32) * SHAPES[name][0] ** -0.5 * times[name]).astype(jnp.bfloat16)
    return drawn


def matmul(a, w):
    return jnp.dot(a, w, preferred_element_type=jnp.float32).astype(jnp.bfloat16)


def normed(h):
    wide = h.astype(jnp.float32)
    scale = lax.rsqrt(jnp.mean(wide**2, -1, keepdims=True) + 1e-6)
    return (wide * scale).astype(jnp.bfloat16)


def turned(t, theta):
    half = t.shape[-1] // 2
    angle = jnp.arange(t.shape[0], dtype=jnp.float32)[:, None] * theta ** (-jnp.arange(half, dtype=jnp.float32) / half)
    cos, sin = jnp.cos(angle)[:, None], jnp.sin(angle)[:, None]
    a, b = t[..., :half].astype(jnp.float32), t[..., half:].astype(jnp.float32)
    return jnp.concatenate([a * cos - b * sin, b * cos + a * sin], -1).astype(jnp.bfloat16)


def seen_by(q, k, v):
    tokens, kv = q.shape[0], k.shape[1]
    q = q.reshape(tokens, kv, -1, q.shape[-1])
    scores = jnp.einsum("tgsd,ugd->gstu", q.astype(jnp.float32), k.astype(jnp.float32)) * q.shape[-1] ** -0.5
    place = jnp.arange(tokens)
    weights = jax.nn.softmax(jnp.where(place[:, None] >= place, scores, -jnp.inf), -1).astype(jnp.bfloat16)
    return jnp.einsum("gstu,ugd->tgsd", weights.astype(jnp.float32), v.astype(jnp.float32)).astype(jnp.bfloat16).reshape(tokens, -1)


def layer(h, w):
    a = normed(h)
    q, k = (turned(matmul(a, w[name]).reshape(h.shape[0], -1, HEAD), THETA) for name in ("wq", "wk"))
    h = h + matmul(seen_by(q, k, matmul(a, w["wv"]).reshape(h.shape[0], -1, HEAD)), w["wo"])
    b = normed(h)
    gate = jnp.dot(b, w["w_gate"], preferred_element_type=jnp.float32)
    up = jnp.dot(b, w["w_up"], preferred_element_type=jnp.float32)
    return h + matmul((jax.nn.silu(gate) * up).astype(jnp.bfloat16), w["w_down"])


def reference(x, dy, wq, wk, wv, wo, w_gate, w_up, w_down):
    weights = dict(zip(NAMES, (wq, wk, wv, wo, w_gate, w_up, w_down), strict=True))

    def take(so_far, sequence):
        h, by_y = sequence
        _, back = jax.vjp(lambda w, h: layer(h, w), weights, h)
        by_weights, by_h = back(by_y)
        return jax.tree.map(lambda total, term: total + term.astype(jnp.float32), so_far, by_weights), by_h

    none_yet = {name: jnp.zeros(w.shape, jnp.float32) for name, w in weights.items()}
    by_weights, by_x = lax.scan(take, none_yet, (x, dy))
    return (by_x, *(by_weights[name].astype(jnp.bfloat16) for name in NAMES))
```

```python
import functools

import jax
import jax.numpy as jnp
from jax import lax
from jax.experimental import pallas as pl
from jax.experimental.pallas import tpu as pltpu
from jax.sharding import PartitionSpec as P

NEG = -1e30
HIDDEN = 2 * NEG
LOG2E = 1.4426950408889634
VMEM = 60 * 2**20
HEAD = 128
THETA = 10000
F32, BF16 = jnp.float32, jnp.bfloat16
N = 512
C = 256


def dot(a, b, ca=1, cb=0):
    return lax.dot_general(a, b, (((ca,), (cb,)), ((), ())), preferred_element_type=F32)


def wide(a):
    return a.astype(F32)


def _attend(pos_ref, q_ref, k_ref, v_ref, o_ref, lse_ref, top_s, mix_s, gap_s, *, scale):
    g, bq, d = q_ref.shape
    cols, bk = g * bq, N
    iq, me = pl.program_id(0), pos_ref[0]
    e = scale * LOG2E
    strips = range(0, cols, N)

    @pl.when(iq == 0)
    def _():
        gap_s[...] = lax.broadcasted_iota(jnp.int32, (bk, bq), 1) - lax.broadcasted_iota(jnp.int32, (bk, bq), 0)

    top_s[...] = jnp.full(top_s.shape, NEG, F32)
    mix_s[...] = jnp.zeros(mix_s.shape, F32)
    ones = jnp.ones((8, bk), BF16)

    def block(j, masked):
        here = pl.ds(jnp.bitwise_xor(j, me) * bk, bk)
        keys = k_ref[here, :]
        scores = [dot(keys, q_ref[...].reshape(cols, d)[at : at + N, :], 1, 1) for at in strips]
        ok = gap_s[...] >= 0 if masked else None
        weights, keeps = [], []
        for at, s in zip(strips, scores):
            if masked:
                s = jnp.where(ok, s, HIDDEN)
            old = top_s[:, at : at + N]
            top = jnp.maximum(old, s.max(axis=0, keepdims=True))
            top_s[:, at : at + N] = top
            weights.append(jnp.exp2((s - top) * e).astype(BF16))
            keeps.append(jnp.exp2((old - top) * e))
        values = jnp.concatenate([v_ref[here, :].T, ones], axis=0)
        for at, p, keep in zip(strips, weights, keeps):
            mix_s[:, at : at + N] = mix_s[:, at : at + N] * keep + dot(values, p, 1, 0)

    lax.fori_loop(0, iq, lambda j, _: block(j, False), None)
    block(iq, True)
    top, total = top_s[...], mix_s[d : d + 1, :]
    o_ref[...] = (mix_s[:d, :] * (1 / total)).T.reshape(g, bq, d).astype(BF16)
    lse = top * scale + jnp.log(total)
    for n in range(g):
        lse_ref[n : n + 1, :] = lse[:, n * bq : (n + 1) * bq]


def attend(q, k, v, me):
    g, t, d = q.shape
    bq = N
    here = lambda i, pos: (0, jnp.bitwise_xor(i, pos[0]), 0)
    whole = pl.BlockSpec((t, d), lambda i, pos: (0, 0))
    return pl.pallas_call(
        functools.partial(_attend, scale=d**-0.5),
        grid_spec=pltpu.PrefetchScalarGridSpec(
            num_scalar_prefetch=1,
            grid=(t // bq,),
            in_specs=[pl.BlockSpec((g, bq, d), here), whole, whole],
            out_specs=[pl.BlockSpec((g, bq, d), here), pl.BlockSpec((g, bq), lambda i, pos: here(i, pos)[:2])],
            scratch_shapes=[pltpu.VMEM((1, g * bq), F32), pltpu.VMEM((d + 8, g * bq), F32), pltpu.VMEM((N, N), jnp.int32)],
        ),
        out_shape=[jax.ShapeDtypeStruct((g, t, d), BF16), jax.ShapeDtypeStruct((g, t), F32)],
        compiler_params=pltpu.CompilerParams(dimension_semantics=("arbitrary",), vmem_limit_bytes=VMEM),
        cost_estimate=pl.CostEstimate(flops=24 * 10**9, transcendentals=g * t * t, bytes_accessed=8 * g * t * d),
        name="attend",
    )(me[None], q, k, v)


def _attend_back(pos_ref, q_ref, k_ref, v_ref, do_ref, lse_ref, delta_ref, dq_ref, dk_ref, dv_ref, dq_s, dk_s, dv_s, gap_s, *, scale):
    g, bq, d = q_ref.shape
    cols, bk = g * bq, N
    iq, me = pl.program_id(0), pos_ref[0]
    e = scale * LOG2E
    strips = range(0, cols, N)

    @pl.when(iq == 0)
    def _():
        gap_s[...] = lax.broadcasted_iota(jnp.int32, (bk, bq), 1) - lax.broadcasted_iota(jnp.int32, (bk, bq), 0)
        dk_s[...] = jnp.zeros_like(dk_s)
        dv_s[...] = jnp.zeros_like(dv_s)

    dq_s[...] = jnp.zeros_like(dq_s)
    lses = [lse_ref[n : n + 1, :] * LOG2E for n in range(g)]
    deltas = [delta_ref[n : n + 1, :] for n in range(g)]

    def block(j, masked):
        here = pl.ds(jnp.bitwise_xor(j, me) * bk, bk)
        keys = k_ref[here, :]
        qs = [q_ref[n] for n in range(g)]
        dos = [do_ref[n] for n in range(g)]
        scores = [dot(keys, x, 1, 1) for x in qs]
        dps = [dot(v_ref[here, :], x, 1, 1) for x in dos]
        ok = gap_s[...] >= 0 if masked else None
        for n, at in enumerate(strips):
            p = jnp.exp2(scores[n] * e - lses[n])
            if masked:
                p = jnp.where(ok, p, 0.0)
            ds = (p * (dps[n] - deltas[n])).astype(BF16)
            dv_s[here, :] += dot(p.astype(BF16), dos[n], 1, 0)
            dk_s[here, :] += dot(ds, qs[n], 1, 0)
            dq_s[:, at : at + N] += dot(keys.T, ds, 1, 0)

    lax.fori_loop(0, iq, lambda j, _: block(j, False), None)
    block(iq, True)
    dq_ref[...] = (dq_s[...] * scale).T.reshape(g, bq, d).astype(BF16)

    @pl.when(iq == pl.num_programs(0) - 1)
    def _():
        dk_ref[...] = (dk_s[...] * scale).astype(BF16)
        dv_ref[...] = dv_s[...].astype(BF16)


def attend_back(q, k, v, d_out, lse, delta, me):
    g, t, d = q.shape
    here = lambda i, pos: (0, jnp.bitwise_xor(i, pos[0]), 0)
    queries = pl.BlockSpec((g, N, d), here)
    stats = pl.BlockSpec((g, N), lambda i, pos: here(i, pos)[:2])
    whole = pl.BlockSpec((t, d), lambda i, pos: (0, 0))
    return pl.pallas_call(
        functools.partial(_attend_back, scale=d**-0.5),
        grid_spec=pltpu.PrefetchScalarGridSpec(
            num_scalar_prefetch=1,
            grid=(t // N,),
            in_specs=[queries, whole, whole, queries, stats, stats],
            out_specs=[queries, whole, whole],
            scratch_shapes=[pltpu.VMEM((d, g * N), F32), pltpu.VMEM((t, d), F32), pltpu.VMEM((t, d), F32), pltpu.VMEM((N, N), jnp.int32)],
        ),
        out_shape=[jax.ShapeDtypeStruct((g, t, d), BF16), jax.ShapeDtypeStruct((t, d), BF16), jax.ShapeDtypeStruct((t, d), BF16)],
        compiler_params=pltpu.CompilerParams(dimension_semantics=("arbitrary",), vmem_limit_bytes=VMEM),
        cost_estimate=pl.CostEstimate(flops=33 * 10**9, transcendentals=g * t * t, bytes_accessed=14 * g * t * d),
        name="attend_back",
    )(me[None], q, k, v, d_out, lse, delta)


def tokens(r=0):
    return lambda i: (i + r, 0)


def fused(body, steps, flops, pieces=(), weights=(), tiles=(), outs=(), into=(), cuts=(), lazy=False):
    flat = [a for piece in pieces for a in piece] + [a for weight in weights for a, _ in weight]
    heights = [sum(a.shape[0] for a, _ in weight) for weight in weights]
    edges = [(0, *cuts, weight[0][0].shape[1]) for weight in weights]
    n_copies = sum(len(piece) for piece in pieces) + sum(len(weight) * (len(e) - 1) for weight, e in zip(weights, edges))

    def kernel(*refs):
        i = pl.program_id(0)
        place = lax.axis_index("dp")
        given, refs = refs[: len(flat)], refs[len(flat) :]
        tile_refs, refs = refs[: len(tiles)], refs[len(tiles) + len(into) :]
        out_refs, refs = refs[: len(outs)], refs[len(outs) :]
        piece_refs, weight_refs, sem = refs[: len(pieces)], refs[len(pieces) : -1], refs[-1]
        copies, n = [], 0
        for piece, ref in zip(pieces, piece_refs):
            for s in range(len(piece)):
                copies.append(pltpu.make_async_copy(given[n], ref.at[s], sem.at[n]))
                n += 1
        slots, parts = n, []
        for w, (weight, ref, edge) in enumerate(zip(weights, weight_refs, edges)):
            for lo, hi in zip(edge, edge[1:]):
                for m, (a, row) in enumerate(weight):
                    known = not callable(row)
                    row = row if known else row(place)
                    copy = pltpu.make_async_copy(given[n + m].at[:, lo:hi], ref.at[pl.ds(row, a.shape[0]), lo:hi], sem.at[slots])
                    parts.append((lo, w, row if known else None, a.shape[0], lo, hi, copy))
                    slots += 1
            n += len(weight)
        parts.sort(key=lambda part: part[0])

        @pl.when(i == 0)
        def _():
            for p in range(len(pieces)):
                copies[p * steps].start()
            for part in parts:
                part[-1].start()
            for p in range(len(pieces)):
                for s in range(1, steps):
                    copies[p * steps + s].start()

        for s in range(steps if pieces else 0):
            @pl.when(i == s)
            def _():
                for p in range(len(pieces)):
                    copies[p * steps + s].wait()

        left = list(parts)

        def need(w, rows, columns):
            now = [part for part in left if part[1] in (w if isinstance(w, tuple) else (w,)) and part[4] < columns[1] and columns[0] < part[5]
                   and (part[2] is None or part[2] < rows[1] and rows[0] < part[2] + part[3])]
            if lazy and now:
                now = now if len(left) == len(parts) else list(left)
            elif now:
                now = list(left)
            for part in now:
                left.remove(part)
            if now:
                @pl.when(i == 0)
                def _():
                    for part in now:
                        part[-1].wait()

        body(i, piece_refs, weight_refs, tile_refs, out_refs, need)
        assert not left

    size = lambda shape, dtype: functools.reduce(lambda p, q: p * q, shape, 1) * jnp.dtype(dtype).itemsize
    moved = sum(size(a.shape, a.dtype) for a in flat) + sum(size(a.shape, a.dtype) for a, _, _ in tiles)
    return pl.pallas_call(
        kernel,
        grid=(steps,),
        in_specs=[pl.BlockSpec(memory_space=pl.ANY)] * len(flat) + [pl.BlockSpec(b, m) for _, b, m in tiles]
        + [pl.BlockSpec(memory_space=pl.ANY)] * len(into),
        out_specs=[pl.BlockSpec(b, m) for _, _, b, m in outs],
        out_shape=[jax.ShapeDtypeStruct(s, t) for s, t, _, _ in outs],
        input_output_aliases={len(flat) + len(tiles) + n: n for n in range(len(into))},
        scratch_shapes=[
            *(pltpu.VMEM((steps, *piece[0].shape), piece[0].dtype) for piece in pieces),
            *(pltpu.VMEM((h, weight[0][0].shape[1]), weight[0][0].dtype) for h, weight in zip(heights, weights)),
            pltpu.SemaphoreType.DMA((n_copies,)),
        ],
        compiler_params=pltpu.CompilerParams(dimension_semantics=("arbitrary",), vmem_limit_bytes=VMEM),
        cost_estimate=pl.CostEstimate(flops=int(flops * 1.3), transcendentals=0, bytes_accessed=moved),
    )(*flat, *(a for a, _, _ in tiles), *into)


def chunks(width, step):
    for at in range(0, width, C):
        step(at)


def each(i, outs, into):
    for s, out in enumerate(outs):
        pl.when(i == s)(functools.partial(into, out))


def by_distance(blocks):
    n = blocks[0].shape[0]
    return [(b, at) for b, at in zip(blocks, (0, *range(n, 4 * n, n // 2)))]


def by_place(blocks):
    n = blocks[0].shape[0]
    at = lambda r, more=0: lambda place: pl.multiple_of(jnp.bitwise_xor(place, r) * n + more, n // 2)
    return [(b, f) for b, f in zip(blocks, (at(0), *(at(r, more) for r in (1, 2, 3) for more in (0, n // 2))))]


def swap(a, axis, bit):
    return lax.ppermute(a, axis, [(i, i ^ bit) for i in range(4)])


def dp_gather(block):
    half = block.shape[0] // 2
    top, low = block[:half], block[half:]
    y_top, z_low = swap(top, "dp", 2), swap(low, "dp", 1)
    y_low, z_top = swap(low, "dp", 2), swap(top, "dp", 1)
    return [block, z_top, z_low, y_top, y_low, swap(y_top, "dp", 1), swap(z_low, "dp", 2)]


def finish(own, top, low, columns):
    n, c = own.shape
    half = n // 2
    halved = isinstance(top, list)
    given = [*top, *low] if halved else [top, low]

    def kernel(own_ref, *refs):
        given_refs, outs = refs[: len(given)], refs[len(given) :]

        def add(refs):
            total = wide(own_ref[...])
            for ref in refs:
                total += wide(ref[...])
            at = 0
            for out in outs:
                out[...] = total[:, at : at + out.shape[1]].astype(BF16)
                at += out.shape[1]

        if halved:
            for s in range(2):
                pl.when(pl.program_id(0) == s)(functools.partial(add, given_refs[2 * s : 2 * s + 2]))
        else:
            add(given_refs)

    return pl.pallas_call(
        kernel,
        grid=(2,),
        in_specs=[pl.BlockSpec((half, c), tokens())] + [pl.BlockSpec((half, c), (lambda i: (0, 0)) if halved else tokens())] * len(given),
        out_specs=[pl.BlockSpec((half, w), tokens()) for w in columns],
        out_shape=[jax.ShapeDtypeStruct((n, w), BF16) for w in columns],
        compiler_params=pltpu.CompilerParams(dimension_semantics=("arbitrary",), vmem_limit_bytes=30 * 2**20),
        cost_estimate=pl.CostEstimate(flops=10**9, transcendentals=0, bytes_accessed=8 * n * c),
    )(own, *given)


def dp_scatter(term, middle, columns):
    d = term(3)
    half = d.shape[0] // 2
    by_y, by_z = swap(d[:half], "dp", 2), swap(d[half:], "dp", 1)
    z, y = middle()
    z_low = swap(z[half:], "dp", 1)
    z_top = swap((wide(z[:half]) + wide(by_y)).astype(BF16), "dp", 1)
    y_top = swap(y[:half], "dp", 2)
    y_low = swap((wide(y[half:]) + wide(by_z)).astype(BF16), "dp", 2)
    own = term(0)
    return finish(own, [z_top, y_top], [z_low, y_low], columns)


def dp_scatter_by(way, term, columns):
    other = 3 - way
    d = term(3)
    far = swap(d, "dp", way)
    near = term(way)
    near = swap(near, "dp", way)
    far = (wide(term(other)) + wide(far)).astype(BF16)
    far = swap(far, "dp", other)
    own = term(0)
    return finish(own, near, far, columns)


def tp_gather(block):
    x = swap(block, "tp", 2)
    near = swap(block, "tp", 1)
    far = swap(x, "tp", 1)
    return [block, near, x, far]


def tp_scatter(far, near):
    far_in = swap(far[1], "tp", 1)
    out = (wide(far[0]) + wide(far_in)).astype(BF16)
    back = swap(out, "tp", 2)
    near_in = swap(near[1], "tp", 1)
    return near[0], near_in, back


def rms(h):
    return lax.rsqrt(jnp.mean(wide(h) ** 2, -1, keepdims=True) + 1e-6)


def normed(h):
    return (wide(h) * rms(h)).astype(BF16)


def normed_back(given, h, more):
    n, d = h.shape
    size = n // 4

    def kernel(*refs):
        *given_refs, h_ref, more_ref, out = refs
        total = wide(given_refs[0][...])
        for ref in given_refs[1:]:
            total += wide(ref[...])
        total = wide(total.astype(BF16))
        w = wide(h_ref[...])
        s = lax.rsqrt(jnp.mean(w**2, -1, keepdims=True) + 1e-6)
        out[...] = (wide(more_ref[...]) + s * total - w * (s**3 * jnp.mean(total * w, -1, keepdims=True))).astype(BF16)

    return pl.pallas_call(
        kernel,
        grid=(n // size,),
        in_specs=[pl.BlockSpec((size, d), tokens())] * (len(given) + 2),
        out_specs=pl.BlockSpec((size, d), tokens()),
        out_shape=jax.ShapeDtypeStruct((n, d), BF16),
        compiler_params=pltpu.CompilerParams(dimension_semantics=("arbitrary",), vmem_limit_bytes=VMEM),
        cost_estimate=pl.CostEstimate(flops=10**9, transcendentals=n, bytes_accessed=12 * n * d),
    )(*given, h, more)


def angles_of(me, t):
    at = (jnp.arange(t, dtype=jnp.int32) ^ (me * N)).astype(F32)
    half = HEAD // 2
    angle = at[:, None] * THETA ** (-jnp.arange(half, dtype=F32) / half)
    cos, sin = jnp.cos(angle), jnp.sin(angle)
    return jnp.concatenate([cos, cos], 1), jnp.concatenate([-sin, sin], 1)


def place_of(at, size):
    return pl.multiple_of(jnp.bitwise_xor(lax.axis_index("dp"), at // size) * size + at % size, C)


def keep_by_distance(out, piece):
    size = out.shape[1] // 4
    for at in range(0, 4 * size, size):
        out[:, at : at + size] = piece[:, pl.ds(place_of(at, size), size)]


def solution(mesh):
    def step(x, dy, wq, wk, wv, wo, w_gate, w_up, w_down):
        place, me = lax.axis_index("dp"), lax.axis_index("tp")
        x, dy = x[0], dy[0]
        d = x.shape[1]
        t = 4 * N
        nq, nk, ff = wq.shape[1], wk.shape[1], w_gate.shape[1]
        width = nq + 2 * nk
        heads = nq // HEAD
        row = lambda c, dtype=BF16: ((t, c), dtype, (N, c), tokens())
        pair = [((N, d), BF16, (N, d), lambda i: (0, 0))] * 2

        w_qkv = dp_gather(jnp.concatenate([wq, wk, wv], 1))
        w_o = dp_gather(wo)
        w_d = dp_gather(w_down)
        w_g = dp_gather(w_gate)
        w_u = dp_gather(w_up)

        cos, sin = angles_of(me, t)
        half = HEAD // 2

        a = tp_gather(normed(x))
        dys = tp_gather(dy)

        def qkv(i, pieces, weights, tiles, outs, need):
            cos, sin = (ref[...] for ref in tiles)
            q, k, v, kept = outs
            need(0, (0, d), (0, width))
            for n in range(width // HEAD):
                if n % 2 == 0:
                    two = dot(pieces[0][i], weights[0][:, n * HEAD : (n + 2) * HEAD]).astype(BF16)
                one = two[:, n % 2 * HEAD : (n % 2 + 1) * HEAD]
                if n <= heads:
                    one = wide(one)
                    one = (one * cos + pltpu.roll(one, half, 1) * sin).astype(BF16)
                if n < heads:
                    q[n] = one
                elif n == heads:
                    k[...] = one
                else:
                    v[...] = one
            keep_by_distance(kept, pieces[0].at[i])

        by_head = lambda r=0: ((heads, N, HEAD), lambda i: (0, i + r, 0))
        angles = [(cos, (N, HEAD), tokens()), (sin, (N, HEAD), tokens())]
        q, k, v, a_all = fused(qkv, 4, 2 * t * d * width, [a], [by_place(w_qkv)], angles,
                               [((heads, t, HEAD), BF16, *by_head()), row(HEAD), row(HEAD), row(d)])
        o, lse = attend(q, k, v, me)

        def project(i, pieces, weights, tiles, outs, need):
            def into(out):
                need(0, (0, nq), (0, d))
                o = jnp.concatenate([tiles[0][n] for n in range(heads)], 1)

                def one(at):
                    out[:, pl.ds(at, C)] = dot(o, weights[0][:, pl.ds(at, C)]).astype(BF16)

                chunks(d, one)

            each(i, outs, into)

        far, near = (fused(project, 2, t * d * nq, [], [by_place(w_o)], [(o, *by_head(r))], pair) for r in (2, 0))
        h = tp_scatter(far, near)
        h = x + sum(wide(part) for part in h).astype(BF16)
        b = normed(h)
        b = tp_gather(b)

        def down(i, pieces, weights, tiles, outs, need):
            need(0, (0, ff), (0, d))

            def one(at):
                outs[0][:, pl.ds(at, C)] = dot(pieces[0][i], weights[0][pl.ds(at, C), :], 1, 1).astype(BF16)

            chunks(ff, one)
            outs[1][...] = pieces[0][i]

        d_hidden, dy_all = fused(down, 4, 2 * t * d * ff, [dys], [by_place(w_d)], [], [row(ff), row(d)])

        def gated(i, pieces, weights, tiles, outs, need):
            def one(at):
                need(0, (0, d), (at, at + C))
                outs[0][:, pl.ds(at, C)] = dot(pieces[0][i], weights[0][:, pl.ds(at, C)])

            chunks(ff, one)
            keep_by_distance(outs[1], pieces[0].at[i])

        kept = ()
        for r in (0, 2):
            kept = fused(gated, 2, t * d * ff, [b[r : r + 2]], [by_place(w_g)], [], [((t, ff), F32, (N, ff), tokens(r)), ((t, d), BF16, (N, d), tokens(r))],
                         kept)
        gate, b_all = kept

        def upped(i, pieces, weights, tiles, outs, need):
            def one(at):
                here = pl.ds(at, C)
                need(0, (0, d), (at, at + C))
                up = dot(tiles[0][...], weights[0][:, here])
                gate, dh = tiles[1][:, here], wide(tiles[2][:, here])
                sig = 1 / (1 + jnp.exp(-gate))
                silu = gate * sig
                outs[0][:, here] = (silu * up).astype(BF16)
                outs[1][:, here] = (dh * up * (sig + silu * (1 - sig))).astype(BF16)
                outs[1][:, pl.ds(ff + at, C)] = (dh * silu).astype(BF16)

            chunks(ff, one)

        hidden, d_both = fused(upped, 4, 2 * t * d * ff, [], [by_distance(w_u)],
                                     [(b_all, (N, d), tokens()), (gate, (N, ff), tokens()), (d_hidden, (N, ff), tokens())], [row(ff), row(2 * ff)])

        def to_b(i, pieces, weights, tiles, outs, need):
            def into(out):
                def one(at):
                    here = pl.ds(at, C)
                    need((0, 1), (at, at + C), (0, ff))
                    out[:, pl.ds(place_of(at, d // 4), C)] = (dot(tiles[0][:, :ff], weights[0][here, :], 1, 1) + dot(tiles[0][:, ff:], weights[1][here, :], 1, 1)).astype(BF16)

                chunks(d, one)

            each(i, outs, into)

        far, near = (fused(to_b, 2, 2 * t * d * ff, [], [by_distance(w_g), by_distance(w_u)],
                           [(d_both, (N, 2 * ff), tokens(r))], pair, lazy=True) for r in (2, 0))
        db = tp_scatter(far, near)
        dw_d = dot(hidden, dy_all, 0, 0).astype(BF16)
        nd = w_down.shape[0]
        pick = lambda t, r, n: lax.dynamic_slice_in_dim(t, (place ^ r) * n, n, 0)
        by_down, = dp_scatter(lambda r: pick(dw_d, r, nd), lambda: (pick(dw_d, 1, nd), pick(dw_d, 2, nd)), [d])
        of = d // 4
        by_b = lambda r, n=1: dot(b_all[:, r * of : (r + n) * of], d_both, 0, 0).astype(BF16)

        def middle():
            two = by_b(1, 2)
            return two[:of], two[of:]

        by_gate, by_up = dp_scatter(by_b, middle, [ff, ff])
        dh = normed_back(db, h, dy)

        dhs = tp_gather(dh)

        def from_o(i, pieces, weights, tiles, outs, need):
            need(0, (0, nq), (0, d))
            for n in range(0, heads, 2):
                two = dot(pieces[0][i], weights[0][n * HEAD : (n + 2) * HEAD, :], 1, 1).astype(BF16)
                outs[0][n], outs[0][n + 1] = two[:, :HEAD], two[:, HEAD:]
                both = wide(two) * jnp.concatenate([wide(tiles[0][n]), wide(tiles[0][n + 1])], 1)
                outs[2][n : n + 1, :] = both[:, :HEAD].T.sum(0, keepdims=True)
                outs[2][n + 1 : n + 2, :] = both[:, HEAD:].T.sum(0, keepdims=True)
            outs[1][...] = pieces[0][i]

        d_o, dh_all, delta = fused(from_o, 4, 2 * t * d * nq, [dhs], [by_place(w_o)], [(o, *by_head())],
                                   [((heads, t, HEAD), BF16, *by_head()), row(d), ((heads, t), F32, (heads, N), lambda i: (0, i))])
        dw_o = lax.dot_general(o, dh_all, (((1,), (0,)), ((), ())), preferred_element_type=F32).astype(BF16).reshape(nq, d)
        by_o, = dp_scatter_by(2, lambda r: pick(dw_o, r, wo.shape[0]), [d])
        dq, dk, dv = attend_back(q, k, v, d_o, lse, delta, me)

        def to_a(i, pieces, weights, tiles, outs, need):
            cos, sin = tiles[3][...], tiles[4][...]
            back = lambda t: (wide(t) * cos - pltpu.roll(wide(t), half, 1) * sin).astype(BF16)
            one = jnp.concatenate([*(back(tiles[0][n]) for n in range(heads)), back(tiles[1][...]), tiles[2][...]], 1)
            outs[2][...] = one

            def into(out):
                def some(at):
                    need(0, (at, at + C), (0, width))
                    out[:, pl.ds(place_of(at, d // 4), C)] = dot(outs[2][...], weights[0][pl.ds(at, C), :], 1, 1).astype(BF16)

                chunks(d, some)

            each(i, outs[:2], into)

        far, near = (fused(to_a, 2, t * d * width, [], [by_distance(w_qkv)],
                           [(dq, *by_head(r)), (dk, (N, HEAD), tokens(r)), (dv, (N, HEAD), tokens(r)), (cos, (N, HEAD), tokens(r)), (sin, (N, HEAD), tokens(r))],
                           [*pair, ((t // 2, width), BF16, (N, width), tokens())]) for r in (2, 0))
        da = tp_scatter(far[:2], near[:2])
        d_qkv = jnp.concatenate([near[2], far[2]], 0)
        by_a = lambda r, n=1: dot(a_all[:, r * of : (r + n) * of], d_qkv, 0, 0).astype(BF16)

        def middle_a():
            two = by_a(1, 2)
            return two[:of], two[of:]

        by_q, by_k, by_v = dp_scatter(by_a, middle_a, [nq, nk, nk])
        dx = normed_back(da, x, dh)
        return dx[None], by_q, by_k, by_v, by_o, by_gate, by_up, by_down

    states, by_columns, by_rows = P("dp", "tp", None), P("dp", "tp"), P(("tp", "dp"), None)
    weights = (by_columns, by_columns, by_columns, by_rows, by_columns, by_columns, by_rows)
    return jax.shard_map(step, mesh=mesh, in_specs=(states, states, *weights), out_specs=(states, *weights), check_vma=False)
```

```python
import functools

import jax
import jax.numpy as jnp
from jax import lax
from jax.experimental import pallas as pl
from jax.experimental.pallas import tpu as pltpu
from jax.sharding import PartitionSpec as P

NEG = -1e30
HIDDEN = 2 * NEG
LOG2E = 1.4426950408889634
VMEM = 60 * 2**20
HEAD = 128
THETA = 10000
F32, BF16 = jnp.float32, jnp.bfloat16
N = 512
C = 256


def dot(a, b, ca=1, cb=0):
    return lax.dot_general(a, b, (((ca,), (cb,)), ((), ())), preferred_element_type=F32)


def wide(a):
    return a.astype(F32)


def _attend(pos_ref, q_ref, k_ref, v_ref, o_ref, lse_ref, top_s, mix_s, gap_s, *, scale):
    g, bq, d = q_ref.shape
    cols, bk = g * bq, N
    iq, me = pl.program_id(0), pos_ref[0]
    e = scale * LOG2E
    strips = range(0, cols, N)

    @pl.when(iq == 0)
    def _():
        gap_s[...] = lax.broadcasted_iota(jnp.int32, (bk, bq), 1) - lax.broadcasted_iota(jnp.int32, (bk, bq), 0)

    top_s[...] = jnp.full(top_s.shape, NEG, F32)
    mix_s[...] = jnp.zeros(mix_s.shape, F32)
    ones = jnp.ones((8, bk), BF16)

    def block(j, masked):
        here = pl.ds(jnp.bitwise_xor(j, me) * bk, bk)
        keys = k_ref[here, :]
        scores = [dot(keys, q_ref[...].reshape(cols, d)[at : at + N, :], 1, 1) for at in strips]
        ok = gap_s[...] >= 0 if masked else None
        weights, keeps = [], []
        for at, s in zip(strips, scores):
            if masked:
                s = jnp.where(ok, s, HIDDEN)
            old = top_s[:, at : at + N]
            top = jnp.maximum(old, s.max(axis=0, keepdims=True))
            top_s[:, at : at + N] = top
            weights.append(jnp.exp2((s - top) * e).astype(BF16))
            keeps.append(jnp.exp2((old - top) * e))
        values = jnp.concatenate([v_ref[here, :].T, ones], axis=0)
        for at, p, keep in zip(strips, weights, keeps):
            mix_s[:, at : at + N] = mix_s[:, at : at + N] * keep + dot(values, p, 1, 0)

    lax.fori_loop(0, iq, lambda j, _: block(j, False), None)
    block(iq, True)
    top, total = top_s[...], mix_s[d : d + 1, :]
    o_ref[...] = (mix_s[:d, :] * (1 / total)).T.reshape(g, bq, d).astype(BF16)
    lse = top * scale + jnp.log(total)
    for n in range(g):
        lse_ref[n : n + 1, :] = lse[:, n * bq : (n + 1) * bq]


def attend(q, k, v, me):
    g, t, d = q.shape
    bq = N
    here = lambda i, pos: (0, jnp.bitwise_xor(i, pos[0]), 0)
    whole = pl.BlockSpec((t, d), lambda i, pos: (0, 0))
    return pl.pallas_call(
        functools.partial(_attend, scale=d**-0.5),
        grid_spec=pltpu.PrefetchScalarGridSpec(
            num_scalar_prefetch=1,
            grid=(t // bq,),
            in_specs=[pl.BlockSpec((g, bq, d), here), whole, whole],
            out_specs=[pl.BlockSpec((g, bq, d), here), pl.BlockSpec((g, bq), lambda i, pos: here(i, pos)[:2])],
            scratch_shapes=[pltpu.VMEM((1, g * bq), F32), pltpu.VMEM((d + 8, g * bq), F32), pltpu.VMEM((N, N), jnp.int32)],
        ),
        out_shape=[jax.ShapeDtypeStruct((g, t, d), BF16), jax.ShapeDtypeStruct((g, t), F32)],
        compiler_params=pltpu.CompilerParams(dimension_semantics=("arbitrary",), vmem_limit_bytes=VMEM),
        cost_estimate=pl.CostEstimate(flops=24 * 10**9, transcendentals=g * t * t, bytes_accessed=8 * g * t * d),
        name="attend",
    )(me[None], q, k, v)


def _attend_back(pos_ref, q_ref, k_ref, v_ref, do_ref, lse_ref, delta_ref, dq_ref, dk_ref, dv_ref, dq_s, dk_s, dv_s, gap_s, *, scale):
    g, bq, d = q_ref.shape
    cols, bk = g * bq, N
    iq, me = pl.program_id(0), pos_ref[0]
    e = scale * LOG2E
    strips = range(0, cols, N)

    @pl.when(iq == 0)
    def _():
        gap_s[...] = lax.broadcasted_iota(jnp.int32, (bk, bq), 1) - lax.broadcasted_iota(jnp.int32, (bk, bq), 0)
        dk_s[...] = jnp.zeros_like(dk_s)
        dv_s[...] = jnp.zeros_like(dv_s)

    dq_s[...] = jnp.zeros_like(dq_s)
    lses = [lse_ref[n : n + 1, :] * LOG2E for n in range(g)]
    deltas = [delta_ref[n : n + 1, :] for n in range(g)]

    def block(j, masked):
        here = pl.ds(jnp.bitwise_xor(j, me) * bk, bk)
        keys = k_ref[here, :]
        qs = [q_ref[n] for n in range(g)]
        dos = [do_ref[n] for n in range(g)]
        scores = [dot(keys, x, 1, 1) for x in qs]
        dps = [dot(v_ref[here, :], x, 1, 1) for x in dos]
        ok = gap_s[...] >= 0 if masked else None
        for n, at in enumerate(strips):
            p = jnp.exp2(scores[n] * e - lses[n])
            if masked:
                p = jnp.where(ok, p, 0.0)
            ds = (p * (dps[n] - deltas[n])).astype(BF16)
            dv_s[here, :] += dot(p.astype(BF16), dos[n], 1, 0)
            dk_s[here, :] += dot(ds, qs[n], 1, 0)
            dq_s[:, at : at + N] += dot(keys.T, ds, 1, 0)

    lax.fori_loop(0, iq, lambda j, _: block(j, False), None)
    block(iq, True)
    dq_ref[...] = (dq_s[...] * scale).T.reshape(g, bq, d).astype(BF16)

    @pl.when(iq == pl.num_programs(0) - 1)
    def _():
        dk_ref[...] = (dk_s[...] * scale).astype(BF16)
        dv_ref[...] = dv_s[...].astype(BF16)


def attend_back(q, k, v, d_out, lse, delta, me):
    g, t, d = q.shape
    here = lambda i, pos: (0, jnp.bitwise_xor(i, pos[0]), 0)
    queries = pl.BlockSpec((g, N, d), here)
    stats = pl.BlockSpec((g, N), lambda i, pos: here(i, pos)[:2])
    whole = pl.BlockSpec((t, d), lambda i, pos: (0, 0))
    return pl.pallas_call(
        functools.partial(_attend_back, scale=d**-0.5),
        grid_spec=pltpu.PrefetchScalarGridSpec(
            num_scalar_prefetch=1,
            grid=(t // N,),
            in_specs=[queries, whole, whole, queries, stats, stats],
            out_specs=[queries, whole, whole],
            scratch_shapes=[pltpu.VMEM((d, g * N), F32), pltpu.VMEM((t, d), F32), pltpu.VMEM((t, d), F32), pltpu.VMEM((N, N), jnp.int32)],
        ),
        out_shape=[jax.ShapeDtypeStruct((g, t, d), BF16), jax.ShapeDtypeStruct((t, d), BF16), jax.ShapeDtypeStruct((t, d), BF16)],
        compiler_params=pltpu.CompilerParams(dimension_semantics=("arbitrary",), vmem_limit_bytes=VMEM),
        cost_estimate=pl.CostEstimate(flops=33 * 10**9, transcendentals=g * t * t, bytes_accessed=14 * g * t * d),
        name="attend_back",
    )(me[None], q, k, v, d_out, lse, delta)


def tokens(r=0):
    return lambda i: (i + r, 0)


def fused(body, steps, flops, pieces=(), weights=(), tiles=(), outs=(), into=(), cuts=(), lazy=False):
    flat = [a for piece in pieces for a in piece] + [a for weight in weights for a, _ in weight]
    heights = [sum(a.shape[0] for a, _ in weight) for weight in weights]
    edges = [(0, *cuts, weight[0][0].shape[1]) for weight in weights]
    n_copies = sum(len(piece) for piece in pieces) + sum(len(weight) * (len(e) - 1) for weight, e in zip(weights, edges))

    def kernel(*refs):
        i = pl.program_id(0)
        place = lax.axis_index("dp")
        given, refs = refs[: len(flat)], refs[len(flat) :]
        tile_refs, refs = refs[: len(tiles)], refs[len(tiles) + len(into) :]
        out_refs, refs = refs[: len(outs)], refs[len(outs) :]
        piece_refs, weight_refs, sem = refs[: len(pieces)], refs[len(pieces) : -1], refs[-1]
        copies, n = [], 0
        for piece, ref in zip(pieces, piece_refs):
            for s in range(len(piece)):
                copies.append(pltpu.make_async_copy(given[n], ref.at[s], sem.at[n]))
                n += 1
        slots, parts = n, []
        for w, (weight, ref, edge) in enumerate(zip(weights, weight_refs, edges)):
            for lo, hi in zip(edge, edge[1:]):
                for m, (a, row) in enumerate(weight):
                    known = not callable(row)
                    row = row if known else row(place)
                    copy = pltpu.make_async_copy(given[n + m].at[:, lo:hi], ref.at[pl.ds(row, a.shape[0]), lo:hi], sem.at[slots])
                    parts.append((lo, w, row if known else None, a.shape[0], lo, hi, copy))
                    slots += 1
            n += len(weight)
        parts.sort(key=lambda part: part[0])

        @pl.when(i == 0)
        def _():
            for p in range(len(pieces)):
                copies[p * steps].start()
            for part in parts:
                part[-1].start()
            for p in range(len(pieces)):
                for s in range(1, steps):
                    copies[p * steps + s].start()

        for s in range(steps if pieces else 0):
            @pl.when(i == s)
            def _():
                for p in range(len(pieces)):
                    copies[p * steps + s].wait()

        left = list(parts)

        def need(w, rows, columns):
            now = [part for part in left if part[1] in (w if isinstance(w, tuple) else (w,)) and part[4] < columns[1] and columns[0] < part[5]
                   and (part[2] is None or part[2] < rows[1] and rows[0] < part[2] + part[3])]
            if lazy and now:
                now = now if len(left) == len(parts) else list(left)
            elif now:
                now = list(left)
            for part in now:
                left.remove(part)
            if now:
                @pl.when(i == 0)
                def _():
                    for part in now:
                        part[-1].wait()

        body(i, piece_refs, weight_refs, tile_refs, out_refs, need)
        assert not left

    size = lambda shape, dtype: functools.reduce(lambda p, q: p * q, shape, 1) * jnp.dtype(dtype).itemsize
    moved = sum(size(a.shape, a.dtype) for a in flat) + sum(size(a.shape, a.dtype) for a, _, _ in tiles)
    return pl.pallas_call(
        kernel,
        grid=(steps,),
        in_specs=[pl.BlockSpec(memory_space=pl.ANY)] * len(flat) + [pl.BlockSpec(b, m) for _, b, m in tiles]
        + [pl.BlockSpec(memory_space=pl.ANY)] * len(into),
        out_specs=[pl.BlockSpec(b, m) for _, _, b, m in outs],
        out_shape=[jax.ShapeDtypeStruct(s, t) for s, t, _, _ in outs],
        input_output_aliases={len(flat) + len(tiles) + n: n for n in range(len(into))},
        scratch_shapes=[
            *(pltpu.VMEM((steps, *piece[0].shape), piece[0].dtype) for piece in pieces),
            *(pltpu.VMEM((h, weight[0][0].shape[1]), weight[0][0].dtype) for h, weight in zip(heights, weights)),
            pltpu.SemaphoreType.DMA((n_copies,)),
        ],
        compiler_params=pltpu.CompilerParams(dimension_semantics=("arbitrary",), vmem_limit_bytes=VMEM),
        cost_estimate=pl.CostEstimate(flops=int(flops * 1.3), transcendentals=0, bytes_accessed=moved),
    )(*flat, *(a for a, _, _ in tiles), *into)


def chunks(width, step):
    for at in range(0, width, C):
        step(at)


def each(i, outs, into):
    for s, out in enumerate(outs):
        pl.when(i == s)(functools.partial(into, out))


def by_distance(blocks):
    n = blocks[0].shape[0]
    return [(b, at) for b, at in zip(blocks, (0, *range(n, 4 * n, n // 2)))]


def by_place(blocks):
    n = blocks[0].shape[0]
    at = lambda r, more=0: lambda place: pl.multiple_of(jnp.bitwise_xor(place, r) * n + more, n // 2)
    return [(b, f) for b, f in zip(blocks, (at(0), *(at(r, more) for r in (1, 2, 3) for more in (0, n // 2))))]


def swap(a, axis, bit):
    return lax.ppermute(a, axis, [(i, i ^ bit) for i in range(4)])


def dp_gather(block):
    half = block.shape[0] // 2
    top, low = block[:half], block[half:]
    y_top, z_low = swap(top, "dp", 2), swap(low, "dp", 1)
    y_low, z_top = swap(low, "dp", 2), swap(top, "dp", 1)
    return [block, z_top, z_low, y_top, y_low, swap(y_top, "dp", 1), swap(z_low, "dp", 2)]


def finish(own, top, low, columns):
    n, c = own.shape
    half = n // 2
    halved = isinstance(top, list)
    given = [*top, *low] if halved else [top, low]

    def kernel(own_ref, *refs):
        given_refs, outs = refs[: len(given)], refs[len(given) :]

        def add(refs):
            total = wide(own_ref[...])
            for ref in refs:
                total += wide(ref[...])
            at = 0
            for out in outs:
                out[...] = total[:, at : at + out.shape[1]].astype(BF16)
                at += out.shape[1]

        if halved:
            for s in range(2):
                pl.when(pl.program_id(0) == s)(functools.partial(add, given_refs[2 * s : 2 * s + 2]))
        else:
            add(given_refs)

    return pl.pallas_call(
        kernel,
        grid=(2,),
        in_specs=[pl.BlockSpec((half, c), tokens())] + [pl.BlockSpec((half, c), (lambda i: (0, 0)) if halved else tokens())] * len(given),
        out_specs=[pl.BlockSpec((half, w), tokens()) for w in columns],
        out_shape=[jax.ShapeDtypeStruct((n, w), BF16) for w in columns],
        compiler_params=pltpu.CompilerParams(dimension_semantics=("arbitrary",), vmem_limit_bytes=30 * 2**20),
        cost_estimate=pl.CostEstimate(flops=10**9, transcendentals=0, bytes_accessed=8 * n * c),
    )(own, *given)


def dp_scatter(term, middle, columns):
    d = term(3)
    half = d.shape[0] // 2
    by_y, by_z = swap(d[:half], "dp", 2), swap(d[half:], "dp", 1)
    z, y = middle()
    z_low = swap(z[half:], "dp", 1)
    z_top = swap((wide(z[:half]) + wide(by_y)).astype(BF16), "dp", 1)
    y_top = swap(y[:half], "dp", 2)
    y_low = swap((wide(y[half:]) + wide(by_z)).astype(BF16), "dp", 2)
    own = term(0)
    return finish(own, [z_top, y_top], [z_low, y_low], columns)


def dp_scatter_by(way, term, columns):
    other = 3 - way
    d = term(3)
    far = swap(d, "dp", way)
    near = term(way)
    near = swap(near, "dp", way)
    far = (wide(term(other)) + wide(far)).astype(BF16)
    far = swap(far, "dp", other)
    own = term(0)
    return finish(own, near, far, columns)


def tp_gather(block):
    x = swap(block, "tp", 2)
    near = swap(block, "tp", 1)
    far = swap(x, "tp", 1)
    return [block, near, x, far]


def tp_scatter(far, near):
    far_in = swap(far[1], "tp", 1)
    out = (wide(far[0]) + wide(far_in)).astype(BF16)
    back = swap(out, "tp", 2)
    near_in = swap(near[1], "tp", 1)
    return near[0], near_in, back


def rms(h):
    return lax.rsqrt(jnp.mean(wide(h) ** 2, -1, keepdims=True) + 1e-6)


def normed(h):
    return (wide(h) * rms(h)).astype(BF16)


def normed_back(given, h, more):
    n, d = h.shape
    size = n // 2

    def kernel(*refs):
        *given_refs, h_ref, more_ref, out = refs
        total = wide(given_refs[0][...])
        for ref in given_refs[1:]:
            total += wide(ref[...])
        total = wide(total.astype(BF16))
        w = wide(h_ref[...])
        s = lax.rsqrt(jnp.mean(w**2, -1, keepdims=True) + 1e-6)
        out[...] = (wide(more_ref[...]) + s * total - w * (s**3 * jnp.mean(total * w, -1, keepdims=True))).astype(BF16)

    return pl.pallas_call(
        kernel,
        grid=(n // size,),
        in_specs=[pl.BlockSpec((size, d), tokens())] * (len(given) + 2),
        out_specs=pl.BlockSpec((size, d), tokens()),
        out_shape=jax.ShapeDtypeStruct((n, d), BF16),
        compiler_params=pltpu.CompilerParams(dimension_semantics=("arbitrary",), vmem_limit_bytes=VMEM),
        cost_estimate=pl.CostEstimate(flops=10**9, transcendentals=n, bytes_accessed=12 * n * d),
    )(*given, h, more)


def angles_of(me, t):
    at = (jnp.arange(t, dtype=jnp.int32) ^ (me * N)).astype(F32)
    half = HEAD // 2
    angle = at[:, None] * THETA ** (-jnp.arange(half, dtype=F32) / half)
    cos, sin = jnp.cos(angle), jnp.sin(angle)
    return jnp.concatenate([cos, cos], 1), jnp.concatenate([-sin, sin], 1)


def place_of(at, size):
    return pl.multiple_of(jnp.bitwise_xor(lax.axis_index("dp"), at // size) * size + at % size, C)


def keep_by_distance(out, piece):
    size = out.shape[1] // 4
    for at in range(0, 4 * size, size):
        out[:, at : at + size] = piece[:, pl.ds(place_of(at, size), size)]


def solution(mesh):
    def step(x, dy, wq, wk, wv, wo, w_gate, w_up, w_down):
        place, me = lax.axis_index("dp"), lax.axis_index("tp")
        x, dy = x[0], dy[0]
        d = x.shape[1]
        t = 4 * N
        nq, nk, ff = wq.shape[1], wk.shape[1], w_gate.shape[1]
        width = nq + 2 * nk
        heads = nq // HEAD
        row = lambda c, dtype=BF16: ((t, c), dtype, (N, c), tokens())
        pair = [((N, d), BF16, (N, d), lambda i: (0, 0))] * 2

        w_qkv = dp_gather(jnp.concatenate([wq, wk, wv], 1))
        w_o = dp_gather(wo)
        w_d = dp_gather(w_down)
        w_g = dp_gather(w_gate)
        w_u = dp_gather(w_up)

        cos, sin = angles_of(me, t)
        half = HEAD // 2

        a = normed(x)
        a = tp_gather(a)
        dys = tp_gather(dy)

        def qkv(i, pieces, weights, tiles, outs, need):
            cos, sin = (ref[...] for ref in tiles)
            q, k, v, kept = outs
            need(0, (0, d), (0, width))
            for n in range(width // HEAD):
                if n % 2 == 0:
                    two = dot(pieces[0][i], weights[0][:, n * HEAD : (n + 2) * HEAD]).astype(BF16)
                one = two[:, n % 2 * HEAD : (n % 2 + 1) * HEAD]
                if n <= heads:
                    one = wide(one)
                    one = (one * cos + pltpu.roll(one, half, 1) * sin).astype(BF16)
                if n < heads:
                    q[n] = one
                elif n == heads:
                    k[...] = one
                else:
                    v[...] = one
            keep_by_distance(kept, pieces[0].at[i])

        by_head = lambda r=0: ((heads, N, HEAD), lambda i: (0, i + r, 0))
        whole = lambda c, r, dtype=BF16: ((t, c), dtype, (N, c), tokens(r))
        by_heads = lambda r: ((heads, t, HEAD), BF16, *by_head(r))
        kept = ()
        for r in (0, 2):
            kept = fused(qkv, 2, t * d * width, [a[r : r + 2]], [by_place(w_qkv)], [(cos, (N, HEAD), tokens(r)), (sin, (N, HEAD), tokens(r))],
                         [by_heads(r), whole(HEAD, r), whole(HEAD, r), whole(d, r)], kept)
        q, k, v, a_all = kept
        o, lse = attend(q, k, v, me)

        def project(i, pieces, weights, tiles, outs, need):
            def into(out):
                need(0, (0, nq), (0, d))
                o = jnp.concatenate([tiles[0][n] for n in range(heads)], 1)

                def one(at):
                    out[:, pl.ds(at, C)] = dot(o, weights[0][:, pl.ds(at, C)]).astype(BF16)

                chunks(d, one)

            each(i, outs, into)

        far, near = (fused(project, 2, t * d * nq, [], [by_place(w_o)], [(o, *by_head(r))], pair) for r in (2, 0))
        h = tp_scatter(far, near)
        h = x + sum(wide(part) for part in h).astype(BF16)
        b = normed(h)
        b = tp_gather(b)

        def down(i, pieces, weights, tiles, outs, need):
            need(0, (0, ff), (0, d))

            def one(at):
                outs[0][:, pl.ds(at, C)] = dot(pieces[0][i], weights[0][pl.ds(at, C), :], 1, 1).astype(BF16)

            chunks(ff, one)
            outs[1][...] = pieces[0][i]

        d_hidden, dy_all = fused(down, 4, 2 * t * d * ff, [dys], [by_place(w_d)], [], [row(ff), row(d)])

        def gated(i, pieces, weights, tiles, outs, need):
            def one(at):
                need(0, (0, d), (at, at + C))
                outs[0][:, pl.ds(at, C)] = dot(pieces[0][i], weights[0][:, pl.ds(at, C)])

            chunks(ff, one)
            keep_by_distance(outs[1], pieces[0].at[i])

        kept = ()
        for r in (0, 2):
            kept = fused(gated, 2, t * d * ff, [b[r : r + 2]], [by_place(w_g)], [], [((t, ff), F32, (N, ff), tokens(r)), ((t, d), BF16, (N, d), tokens(r))],
                         kept)
        gate, b_all = kept

        def upped(i, pieces, weights, tiles, outs, need):
            def one(at):
                here = pl.ds(at, C)
                need(0, (0, d), (at, at + C))
                up = dot(tiles[0][...], weights[0][:, here])
                gate, dh = tiles[1][:, here], wide(tiles[2][:, here])
                sig = 1 / (1 + jnp.exp(-gate))
                silu = gate * sig
                outs[0][:, here] = (silu * up).astype(BF16)
                outs[1][:, here] = (dh * up * (sig + silu * (1 - sig))).astype(BF16)
                outs[1][:, pl.ds(ff + at, C)] = (dh * silu).astype(BF16)

            chunks(ff, one)

        few = N // 2
        narrow = lambda c: ((t, c), BF16, (few, c), tokens())
        hidden, d_both = fused(upped, 8, 2 * t * d * ff, [], [by_distance(w_u)],
                                     [(b_all, (few, d), tokens()), (gate, (few, ff), tokens()), (d_hidden, (few, ff), tokens())], [narrow(ff), narrow(2 * ff)])

        def to_b(i, pieces, weights, tiles, outs, need):
            def into(out):
                def one(at):
                    here = pl.ds(at, C)
                    need((0, 1), (at, at + C), (0, ff))
                    out[:, pl.ds(place_of(at, d // 4), C)] = (dot(tiles[0][:, :ff], weights[0][here, :], 1, 1) + dot(tiles[0][:, ff:], weights[1][here, :], 1, 1)).astype(BF16)

                chunks(d, one)

            each(i, outs, into)

        far, near = (fused(to_b, 2, 2 * t * d * ff, [], [by_distance(w_g), by_distance(w_u)],
                           [(d_both, (N, 2 * ff), tokens(r))], pair, lazy=True) for r in (2, 0))
        db = tp_scatter(far, near)
        dw_d = dot(hidden, dy_all, 0, 0).astype(BF16)
        nd = w_down.shape[0]
        pick = lambda t, r, n: lax.dynamic_slice_in_dim(t, (place ^ r) * n, n, 0)
        by_down, = dp_scatter(lambda r: pick(dw_d, r, nd), lambda: (pick(dw_d, 1, nd), pick(dw_d, 2, nd)), [d])
        of = d // 4
        by_b = lambda r, n=1: dot(b_all[:, r * of : (r + n) * of], d_both, 0, 0).astype(BF16)

        def middle():
            two = by_b(1, 2)
            return two[:of], two[of:]

        by_gate, by_up = dp_scatter(by_b, middle, [ff, ff])
        dh = normed_back(db, h, dy)

        dhs = tp_gather(dh)

        def from_o(i, pieces, weights, tiles, outs, need):
            need(0, (0, nq), (0, d))
            for n in range(0, heads, 2):
                two = dot(pieces[0][i], weights[0][n * HEAD : (n + 2) * HEAD, :], 1, 1).astype(BF16)
                outs[0][n], outs[0][n + 1] = two[:, :HEAD], two[:, HEAD:]
                both = wide(two) * jnp.concatenate([wide(tiles[0][n]), wide(tiles[0][n + 1])], 1)
                outs[2][n : n + 1, :] = both[:, :HEAD].T.sum(0, keepdims=True)
                outs[2][n + 1 : n + 2, :] = both[:, HEAD:].T.sum(0, keepdims=True)
            outs[1][...] = pieces[0][i]

        kept = ()
        for r in (0, 2):
            kept = fused(from_o, 2, t * d * nq, [dhs[r : r + 2]], [by_place(w_o)], [(o, *by_head(r))],
                         [by_heads(r), whole(d, r), ((heads, t), F32, (heads, N), lambda i, r=r: (0, i + r))], kept)
        d_o, dh_all, delta = kept
        dw_o = lax.dot_general(o, dh_all, (((1,), (0,)), ((), ())), preferred_element_type=F32).astype(BF16).reshape(nq, d)
        by_o, = dp_scatter_by(2, lambda r: pick(dw_o, r, wo.shape[0]), [d])
        dq, dk, dv = attend_back(q, k, v, d_o, lse, delta, me)

        def to_a(i, pieces, weights, tiles, outs, need):
            cos, sin = tiles[3][...], tiles[4][...]
            back = lambda t: (wide(t) * cos - pltpu.roll(wide(t), half, 1) * sin).astype(BF16)
            one = jnp.concatenate([*(back(tiles[0][n]) for n in range(heads)), back(tiles[1][...]), tiles[2][...]], 1)
            outs[2][...] = one

            def into(out):
                def some(at):
                    need(0, (at, at + C), (0, width))
                    out[:, pl.ds(place_of(at, d // 4), C)] = dot(outs[2][...], weights[0][pl.ds(at, C), :], 1, 1).astype(BF16)

                chunks(d, some)

            each(i, outs[:2], into)

        far, near = (fused(to_a, 2, t * d * width, [], [by_distance(w_qkv)],
                           [(dq, *by_head(r)), (dk, (N, HEAD), tokens(r)), (dv, (N, HEAD), tokens(r)), (cos, (N, HEAD), tokens(r)), (sin, (N, HEAD), tokens(r))],
                           [*pair, ((t // 2, width), BF16, (N, width), tokens())]) for r in (2, 0))
        da = tp_scatter(far[:2], near[:2])
        d_qkv = jnp.concatenate([near[2], far[2]], 0)
        by_a = lambda r, n=1: dot(a_all[:, r * of : (r + n) * of], d_qkv, 0, 0).astype(BF16)

        def middle_a():
            two = by_a(1, 2)
            return two[:of], two[of:]

        by_q, by_k, by_v = dp_scatter(by_a, middle_a, [nq, nk, nk])
        dx = normed_back(da, x, dh)
        return dx[None], by_q, by_k, by_v, by_o, by_gate, by_up, by_down

    states, by_columns, by_rows = P("dp", "tp", None), P("dp", "tp"), P(("tp", "dp"), None)
    weights = (by_columns, by_columns, by_columns, by_rows, by_columns, by_columns, by_rows)
    return jax.shard_map(step, mesh=mesh, in_specs=(states, states, *weights), out_specs=(states, *weights), check_vma=False)
```

```python
import functools

import jax
import jax.numpy as jnp
from jax import lax
from jax.experimental import pallas as pl
from jax.experimental.pallas import tpu as pltpu
from jax.sharding import PartitionSpec as P

NEG = -1e30
HIDDEN = 2 * NEG
LOG2E = 1.4426950408889634
VMEM = 60 * 2**20
HEAD = 128
THETA = 10000
F32, BF16 = jnp.float32, jnp.bfloat16
N = 512
C = 256


def dot(a, b, ca=1, cb=0):
    return lax.dot_general(a, b, (((ca,), (cb,)), ((), ())), preferred_element_type=F32)


def wide(a):
    return a.astype(F32)


def _attend(pos_ref, q_ref, k_ref, v_ref, o_ref, lse_ref, top_s, mix_s, gap_s, *, scale):
    g, bq, d = q_ref.shape
    cols, bk = g * bq, N
    iq, me = pl.program_id(0), pos_ref[0]
    e = scale * LOG2E
    strips = range(0, cols, N)

    @pl.when(iq == 0)
    def _():
        gap_s[...] = lax.broadcasted_iota(jnp.int32, (bk, bq), 1) - lax.broadcasted_iota(jnp.int32, (bk, bq), 0)

    top_s[...] = jnp.full(top_s.shape, NEG, F32)
    mix_s[...] = jnp.zeros(mix_s.shape, F32)
    ones = jnp.ones((8, bk), BF16)

    def block(j, masked):
        here = pl.ds(jnp.bitwise_xor(j, me) * bk, bk)
        keys = k_ref[here, :]
        scores = [dot(keys, q_ref[...].reshape(cols, d)[at : at + N, :], 1, 1) for at in strips]
        ok = gap_s[...] >= 0 if masked else None
        weights, keeps = [], []
        for at, s in zip(strips, scores):
            if masked:
                s = jnp.where(ok, s, HIDDEN)
            old = top_s[:, at : at + N]
            top = jnp.maximum(old, s.max(axis=0, keepdims=True))
            top_s[:, at : at + N] = top
            weights.append(jnp.exp2((s - top) * e).astype(BF16))
            keeps.append(jnp.exp2((old - top) * e))
        values = jnp.concatenate([v_ref[here, :].T, ones], axis=0)
        for at, p, keep in zip(strips, weights, keeps):
            mix_s[:, at : at + N] = mix_s[:, at : at + N] * keep + dot(values, p, 1, 0)

    lax.fori_loop(0, iq, lambda j, _: block(j, False), None)
    block(iq, True)
    top, total = top_s[...], mix_s[d : d + 1, :]
    o_ref[...] = (mix_s[:d, :] * (1 / total)).T.reshape(g, bq, d).astype(BF16)
    lse = top * scale + jnp.log(total)
    for n in range(g):
        lse_ref[n : n + 1, :] = lse[:, n * bq : (n + 1) * bq]


def attend(q, k, v, me):
    g, t, d = q.shape
    bq = N
    here = lambda i, pos: (0, jnp.bitwise_xor(i, pos[0]), 0)
    whole = pl.BlockSpec((t, d), lambda i, pos: (0, 0))
    return pl.pallas_call(
        functools.partial(_attend, scale=d**-0.5),
        grid_spec=pltpu.PrefetchScalarGridSpec(
            num_scalar_prefetch=1,
            grid=(t // bq,),
            in_specs=[pl.BlockSpec((g, bq, d), here), whole, whole],
            out_specs=[pl.BlockSpec((g, bq, d), here), pl.BlockSpec((g, bq), lambda i, pos: here(i, pos)[:2])],
            scratch_shapes=[pltpu.VMEM((1, g * bq), F32), pltpu.VMEM((d + 8, g * bq), F32), pltpu.VMEM((N, N), jnp.int32)],
        ),
        out_shape=[jax.ShapeDtypeStruct((g, t, d), BF16), jax.ShapeDtypeStruct((g, t), F32)],
        compiler_params=pltpu.CompilerParams(dimension_semantics=("arbitrary",), vmem_limit_bytes=VMEM),
        cost_estimate=pl.CostEstimate(flops=24 * 10**9, transcendentals=g * t * t, bytes_accessed=8 * g * t * d),
        name="attend",
    )(me[None], q, k, v)


def _attend_back(pos_ref, q_ref, k_ref, v_ref, do_ref, lse_ref, delta_ref, dq_ref, dk_ref, dv_ref, dq_s, dk_s, dv_s, gap_s, *, scale):
    g, bq, d = q_ref.shape
    cols, bk = g * bq, N
    iq, me = pl.program_id(0), pos_ref[0]
    e = scale * LOG2E
    strips = range(0, cols, N)

    @pl.when(iq == 0)
    def _():
        gap_s[...] = lax.broadcasted_iota(jnp.int32, (bk, bq), 1) - lax.broadcasted_iota(jnp.int32, (bk, bq), 0)
        dk_s[...] = jnp.zeros_like(dk_s)
        dv_s[...] = jnp.zeros_like(dv_s)

    dq_s[...] = jnp.zeros_like(dq_s)
    lses = [lse_ref[n : n + 1, :] * LOG2E for n in range(g)]
    deltas = [delta_ref[n : n + 1, :] for n in range(g)]

    def block(j, masked):
        here = pl.ds(jnp.bitwise_xor(j, me) * bk, bk)
        keys = k_ref[here, :]
        qs = [q_ref[n] for n in range(g)]
        dos = [do_ref[n] for n in range(g)]
        scores = [dot(keys, x, 1, 1) for x in qs]
        dps = [dot(v_ref[here, :], x, 1, 1) for x in dos]
        ok = gap_s[...] >= 0 if masked else None
        for n, at in enumerate(strips):
            p = jnp.exp2(scores[n] * e - lses[n])
            if masked:
                p = jnp.where(ok, p, 0.0)
            ds = (p * (dps[n] - deltas[n])).astype(BF16)
            dv_s[here, :] += dot(p.astype(BF16), dos[n], 1, 0)
            dk_s[here, :] += dot(ds, qs[n], 1, 0)
            dq_s[:, at : at + N] += dot(keys.T, ds, 1, 0)

    lax.fori_loop(0, iq, lambda j, _: block(j, False), None)
    block(iq, True)
    dq_ref[...] = (dq_s[...] * scale).T.reshape(g, bq, d).astype(BF16)

    @pl.when(iq == pl.num_programs(0) - 1)
    def _():
        dk_ref[...] = (dk_s[...] * scale).astype(BF16)
        dv_ref[...] = dv_s[...].astype(BF16)


def attend_back(q, k, v, d_out, lse, delta, me):
    g, t, d = q.shape
    here = lambda i, pos: (0, jnp.bitwise_xor(i, pos[0]), 0)
    queries = pl.BlockSpec((g, N, d), here)
    stats = pl.BlockSpec((g, N), lambda i, pos: here(i, pos)[:2])
    whole = pl.BlockSpec((t, d), lambda i, pos: (0, 0))
    return pl.pallas_call(
        functools.partial(_attend_back, scale=d**-0.5),
        grid_spec=pltpu.PrefetchScalarGridSpec(
            num_scalar_prefetch=1,
            grid=(t // N,),
            in_specs=[queries, whole, whole, queries, stats, stats],
            out_specs=[queries, whole, whole],
            scratch_shapes=[pltpu.VMEM((d, g * N), F32), pltpu.VMEM((t, d), F32), pltpu.VMEM((t, d), F32), pltpu.VMEM((N, N), jnp.int32)],
        ),
        out_shape=[jax.ShapeDtypeStruct((g, t, d), BF16), jax.ShapeDtypeStruct((t, d), BF16), jax.ShapeDtypeStruct((t, d), BF16)],
        compiler_params=pltpu.CompilerParams(dimension_semantics=("arbitrary",), vmem_limit_bytes=VMEM),
        cost_estimate=pl.CostEstimate(flops=33 * 10**9, transcendentals=g * t * t, bytes_accessed=14 * g * t * d),
        name="attend_back",
    )(me[None], q, k, v, d_out, lse, delta)


def tokens(r=0):
    return lambda i: (i + r, 0)


def fused(body, steps, flops, pieces=(), weights=(), tiles=(), outs=(), into=(), cuts=(), lazy=False):
    flat = [a for piece in pieces for a in piece] + [a for weight in weights for a, _ in weight]
    heights = [sum(a.shape[0] for a, _ in weight) for weight in weights]
    edges = [(0, *cuts, weight[0][0].shape[1]) for weight in weights]
    n_copies = sum(len(piece) for piece in pieces) + sum(len(weight) * (len(e) - 1) for weight, e in zip(weights, edges))

    def kernel(*refs):
        i = pl.program_id(0)
        place = lax.axis_index("dp")
        given, refs = refs[: len(flat)], refs[len(flat) :]
        tile_refs, refs = refs[: len(tiles)], refs[len(tiles) + len(into) :]
        out_refs, refs = refs[: len(outs)], refs[len(outs) :]
        piece_refs, weight_refs, sem = refs[: len(pieces)], refs[len(pieces) : -1], refs[-1]
        copies, n = [], 0
        for piece, ref in zip(pieces, piece_refs):
            for s in range(len(piece)):
                copies.append(pltpu.make_async_copy(given[n], ref.at[s], sem.at[n]))
                n += 1
        slots, parts = n, []
        for w, (weight, ref, edge) in enumerate(zip(weights, weight_refs, edges)):
            for lo, hi in zip(edge, edge[1:]):
                for m, (a, row) in enumerate(weight):
                    known = not callable(row)
                    row = row if known else row(place)
                    copy = pltpu.make_async_copy(given[n + m].at[:, lo:hi], ref.at[pl.ds(row, a.shape[0]), lo:hi], sem.at[slots])
                    parts.append((lo, w, row if known else None, a.shape[0], lo, hi, copy))
                    slots += 1
            n += len(weight)
        parts.sort(key=lambda part: (part[0], part[2] or 0))

        @pl.when(i == 0)
        def _():
            for p in range(len(pieces)):
                copies[p * steps].start()
            for part in parts:
                part[-1].start()
            for p in range(len(pieces)):
                for s in range(1, steps):
                    copies[p * steps + s].start()

        for s in range(steps if pieces else 0):
            @pl.when(i == s)
            def _():
                for p in range(len(pieces)):
                    copies[p * steps + s].wait()

        left = list(parts)

        def need(w, rows, columns):
            if lazy:
                rows = (rows[0] // N * N, -(-rows[1] // N) * N)
            now = [part for part in left if part[1] in (w if isinstance(w, tuple) else (w,)) and part[4] < columns[1] and columns[0] < part[5]
                   and (part[2] is None or part[2] < rows[1] and rows[0] < part[2] + part[3])]
            if now and not lazy:
                now = list(left)
            for part in now:
                left.remove(part)
            if now:
                @pl.when(i == 0)
                def _():
                    for part in now:
                        part[-1].wait()

        body(i, piece_refs, weight_refs, tile_refs, out_refs, need)
        assert not left

    size = lambda shape, dtype: functools.reduce(lambda p, q: p * q, shape, 1) * jnp.dtype(dtype).itemsize
    moved = sum(size(a.shape, a.dtype) for a in flat) + sum(size(a.shape, a.dtype) for a, _, _ in tiles)
    return pl.pallas_call(
        kernel,
        grid=(steps,),
        in_specs=[pl.BlockSpec(memory_space=pl.ANY)] * len(flat) + [pl.BlockSpec(b, m) for _, b, m in tiles]
        + [pl.BlockSpec(memory_space=pl.ANY)] * len(into),
        out_specs=[pl.BlockSpec(b, m) for _, _, b, m in outs],
        out_shape=[jax.ShapeDtypeStruct(s, t) for s, t, _, _ in outs],
        input_output_aliases={len(flat) + len(tiles) + n: n for n in range(len(into))},
        scratch_shapes=[
            *(pltpu.VMEM((steps, *piece[0].shape), piece[0].dtype) for piece in pieces),
            *(pltpu.VMEM((h, weight[0][0].shape[1]), weight[0][0].dtype) for h, weight in zip(heights, weights)),
            pltpu.SemaphoreType.DMA((n_copies,)),
        ],
        compiler_params=pltpu.CompilerParams(dimension_semantics=("arbitrary",), vmem_limit_bytes=VMEM),
        cost_estimate=pl.CostEstimate(flops=int(flops * 1.3), transcendentals=0, bytes_accessed=moved),
    )(*flat, *(a for a, _, _ in tiles), *into)


def chunks(width, step):
    for at in range(0, width, C):
        step(at)


def each(i, outs, into):
    for s, out in enumerate(outs):
        pl.when(i == s)(functools.partial(into, out))


def by_distance(blocks):
    n = blocks[0].shape[0]
    return [(b, at) for b, at in zip(blocks, (0, *range(n, 4 * n, n // 2)))]


def by_place(blocks):
    n = blocks[0].shape[0]
    at = lambda r, more=0: lambda place: pl.multiple_of(jnp.bitwise_xor(place, r) * n + more, n // 2)
    return [(b, f) for b, f in zip(blocks, (at(0), *(at(r, more) for r in (1, 2, 3) for more in (0, n // 2))))]


def swap(a, axis, bit):
    return lax.ppermute(a, axis, [(i, i ^ bit) for i in range(4)])


def dp_gather(block):
    half = block.shape[0] // 2
    top, low = block[:half], block[half:]
    y_top, z_low = swap(top, "dp", 2), swap(low, "dp", 1)
    y_low, z_top = swap(low, "dp", 2), swap(top, "dp", 1)
    return [block, z_top, z_low, y_top, y_low, swap(y_top, "dp", 1), swap(z_low, "dp", 2)]


def finish(own, top, low, columns):
    n, c = own.shape
    half = n // 2
    halved = isinstance(top, list)
    given = [*top, *low] if halved else [top, low]

    def kernel(own_ref, *refs):
        given_refs, outs = refs[: len(given)], refs[len(given) :]

        def add(refs):
            total = wide(own_ref[...])
            for ref in refs:
                total += wide(ref[...])
            at = 0
            for out in outs:
                out[...] = total[:, at : at + out.shape[1]].astype(BF16)
                at += out.shape[1]

        if halved:
            for s in range(2):
                pl.when(pl.program_id(0) == s)(functools.partial(add, given_refs[2 * s : 2 * s + 2]))
        else:
            add(given_refs)

    return pl.pallas_call(
        kernel,
        grid=(2,),
        in_specs=[pl.BlockSpec((half, c), tokens())] + [pl.BlockSpec((half, c), (lambda i: (0, 0)) if halved else tokens())] * len(given),
        out_specs=[pl.BlockSpec((half, w), tokens()) for w in columns],
        out_shape=[jax.ShapeDtypeStruct((n, w), BF16) for w in columns],
        compiler_params=pltpu.CompilerParams(dimension_semantics=("arbitrary",), vmem_limit_bytes=30 * 2**20),
        cost_estimate=pl.CostEstimate(flops=10**9, transcendentals=0, bytes_accessed=8 * n * c),
    )(own, *given)


def dp_scatter(term, middle, columns):
    d = term(3)
    half = d.shape[0] // 2
    by_y, by_z = swap(d[:half], "dp", 2), swap(d[half:], "dp", 1)
    z, y = middle()
    z_low = swap(z[half:], "dp", 1)
    z_top = swap((wide(z[:half]) + wide(by_y)).astype(BF16), "dp", 1)
    y_top = swap(y[:half], "dp", 2)
    y_low = swap((wide(y[half:]) + wide(by_z)).astype(BF16), "dp", 2)
    own = term(0)
    return finish(own, [z_top, y_top], [z_low, y_low], columns)


def dp_scatter_by(way, term, columns):
    other = 3 - way
    d = term(3)
    far = swap(d, "dp", way)
    near = term(way)
    near = swap(near, "dp", way)
    far = (wide(term(other)) + wide(far)).astype(BF16)
    far = swap(far, "dp", other)
    own = term(0)
    return finish(own, near, far, columns)


def tp_gather(block):
    x = swap(block, "tp", 2)
    near = swap(block, "tp", 1)
    far = swap(x, "tp", 1)
    return [block, near, x, far]


def tp_scatter(far, near):
    far_in = swap(far[1], "tp", 1)
    out = (wide(far[0]) + wide(far_in)).astype(BF16)
    back = swap(out, "tp", 2)
    near_in = swap(near[1], "tp", 1)
    return near[0], near_in, back


def rms(h):
    return lax.rsqrt(jnp.mean(wide(h) ** 2, -1, keepdims=True) + 1e-6)


def normed(h):
    return (wide(h) * rms(h)).astype(BF16)


def normed_back(given, h, more):
    n, d = h.shape
    size = n // 2

    def kernel(*refs):
        *given_refs, h_ref, more_ref, out = refs
        total = wide(given_refs[0][...])
        for ref in given_refs[1:]:
            total += wide(ref[...])
        total = wide(total.astype(BF16))
        w = wide(h_ref[...])
        s = lax.rsqrt(jnp.mean(w**2, -1, keepdims=True) + 1e-6)
        out[...] = (wide(more_ref[...]) + s * total - w * (s**3 * jnp.mean(total * w, -1, keepdims=True))).astype(BF16)

    return pl.pallas_call(
        kernel,
        grid=(n // size,),
        in_specs=[pl.BlockSpec((size, d), tokens())] * (len(given) + 2),
        out_specs=pl.BlockSpec((size, d), tokens()),
        out_shape=jax.ShapeDtypeStruct((n, d), BF16),
        compiler_params=pltpu.CompilerParams(dimension_semantics=("arbitrary",), vmem_limit_bytes=VMEM),
        cost_estimate=pl.CostEstimate(flops=10**9, transcendentals=n, bytes_accessed=12 * n * d),
    )(*given, h, more)


def angles_of(me, t):
    at = (jnp.arange(t, dtype=jnp.int32) ^ (me * N)).astype(F32)
    half = HEAD // 2
    angle = at[:, None] * THETA ** (-jnp.arange(half, dtype=F32) / half)
    cos, sin = jnp.cos(angle), jnp.sin(angle)
    return jnp.concatenate([cos, cos], 1), jnp.concatenate([-sin, sin], 1)


def place_of(at, size):
    return pl.multiple_of(jnp.bitwise_xor(lax.axis_index("dp"), at // size) * size + at % size, C)


def keep_by_distance(out, piece):
    size = out.shape[1] // 4
    for at in range(0, 4 * size, size):
        out[:, at : at + size] = piece[:, pl.ds(place_of(at, size), size)]


def solution(mesh):
    def step(x, dy, wq, wk, wv, wo, w_gate, w_up, w_down):
        place, me = lax.axis_index("dp"), lax.axis_index("tp")
        x, dy = x[0], dy[0]
        d = x.shape[1]
        t = 4 * N
        nq, nk, ff = wq.shape[1], wk.shape[1], w_gate.shape[1]
        width = nq + 2 * nk
        heads = nq // HEAD
        row = lambda c, dtype=BF16: ((t, c), dtype, (N, c), tokens())
        pair = [((N, d), BF16, (N, d), lambda i: (0, 0))] * 2

        w_qkv = dp_gather(jnp.concatenate([wq, wk, wv], 1))
        w_o = dp_gather(wo)
        w_d = dp_gather(w_down)
        w_g = dp_gather(w_gate)
        w_u = dp_gather(w_up)

        cos, sin = angles_of(me, t)
        half = HEAD // 2

        a = normed(x)
        a = tp_gather(a)
        dys = tp_gather(dy)

        def qkv(i, pieces, weights, tiles, outs, need):
            cos, sin = (ref[...] for ref in tiles)
            q, k, v, kept = outs
            need(0, (0, d), (0, width))
            for n in range(width // HEAD):
                if n % 2 == 0:
                    two = dot(pieces[0][i], weights[0][:, n * HEAD : (n + 2) * HEAD]).astype(BF16)
                one = two[:, n % 2 * HEAD : (n % 2 + 1) * HEAD]
                if n <= heads:
                    one = wide(one)
                    one = (one * cos + pltpu.roll(one, half, 1) * sin).astype(BF16)
                if n < heads:
                    q[n] = one
                elif n == heads:
                    k[...] = one
                else:
                    v[...] = one
            keep_by_distance(kept, pieces[0].at[i])

        by_head = lambda r=0: ((heads, N, HEAD), lambda i: (0, i + r, 0))
        whole = lambda c, r, dtype=BF16: ((t, c), dtype, (N, c), tokens(r))
        by_heads = lambda r: ((heads, t, HEAD), BF16, *by_head(r))
        kept = ()
        for r in (0, 2):
            kept = fused(qkv, 2, t * d * width, [a[r : r + 2]], [by_place(w_qkv)], [(cos, (N, HEAD), tokens(r)), (sin, (N, HEAD), tokens(r))],
                         [by_heads(r), whole(HEAD, r), whole(HEAD, r), whole(d, r)], kept)
        q, k, v, a_all = kept
        o, lse = attend(q, k, v, me)

        def project(i, pieces, weights, tiles, outs, need):
            def into(out):
                need(0, (0, nq), (0, d))
                o = jnp.concatenate([tiles[0][n] for n in range(heads)], 1)

                def one(at):
                    out[:, pl.ds(at, C)] = dot(o, weights[0][:, pl.ds(at, C)]).astype(BF16)

                chunks(d, one)

            each(i, outs, into)

        far, near = (fused(project, 2, t * d * nq, [], [by_place(w_o)], [(o, *by_head(r))], pair) for r in (2, 0))
        h = tp_scatter(far, near)
        h = x + sum(wide(part) for part in h).astype(BF16)
        b = normed(h)
        b = tp_gather(b)

        def down(i, pieces, weights, tiles, outs, need):
            need(0, (0, ff), (0, d))

            def one(at):
                outs[0][:, pl.ds(at, C)] = dot(pieces[0][i], weights[0][pl.ds(at, C), :], 1, 1).astype(BF16)

            chunks(ff, one)
            outs[1][...] = pieces[0][i]

        d_hidden, dy_all = fused(down, 4, 2 * t * d * ff, [dys], [by_place(w_d)], [], [row(ff), row(d)])

        def gated(i, pieces, weights, tiles, outs, need):
            def one(at):
                need(0, (0, d), (at, at + C))
                outs[0][:, pl.ds(at, C)] = dot(pieces[0][i], weights[0][:, pl.ds(at, C)])

            chunks(ff, one)
            keep_by_distance(outs[1], pieces[0].at[i])

        kept = ()
        for r in (0, 2):
            kept = fused(gated, 2, t * d * ff, [b[r : r + 2]], [by_place(w_g)], [], [((t, ff), F32, (N, ff), tokens(r)), ((t, d), BF16, (N, d), tokens(r))],
                         kept)
        gate, b_all = kept

        def upped(i, pieces, weights, tiles, outs, need):
            def one(at):
                here = pl.ds(at, C)
                need(0, (0, d), (at, at + C))
                up = dot(tiles[0][...], weights[0][:, here])
                gate, dh = tiles[1][:, here], wide(tiles[2][:, here])
                sig = 1 / (1 + jnp.exp(-gate))
                silu = gate * sig
                outs[0][:, here] = (silu * up).astype(BF16)
                outs[1][:, here] = (dh * up * (sig + silu * (1 - sig))).astype(BF16)
                outs[1][:, pl.ds(ff + at, C)] = (dh * silu).astype(BF16)

            chunks(ff, one)

        few = N // 2
        narrow = lambda c: ((t, c), BF16, (few, c), tokens())
        hidden, d_both = fused(upped, 8, 2 * t * d * ff, [], [by_distance(w_u)],
                                     [(b_all, (few, d), tokens()), (gate, (few, ff), tokens()), (d_hidden, (few, ff), tokens())], [narrow(ff), narrow(2 * ff)])

        def to_b(i, pieces, weights, tiles, outs, need):
            def into(out):
                def one(at):
                    here = pl.ds(at, C)
                    need((0, 1), (at, at + C), (0, ff))
                    out[:, pl.ds(place_of(at, d // 4), C)] = (dot(tiles[0][:, :ff], weights[0][here, :], 1, 1) + dot(tiles[0][:, ff:], weights[1][here, :], 1, 1)).astype(BF16)

                chunks(d, one)

            each(i, outs, into)

        far, near = (fused(to_b, 2, 2 * t * d * ff, [], [by_distance(w_g), by_distance(w_u)],
                           [(d_both, (N, 2 * ff), tokens(r))], pair, lazy=True) for r in (2, 0))
        db = tp_scatter(far, near)
        dw_d = dot(hidden, dy_all, 0, 0).astype(BF16)
        nd = w_down.shape[0]
        pick = lambda t, r, n: lax.dynamic_slice_in_dim(t, (place ^ r) * n, n, 0)
        by_down, = dp_scatter(lambda r: pick(dw_d, r, nd), lambda: (pick(dw_d, 1, nd), pick(dw_d, 2, nd)), [d])
        of = d // 4
        by_b = lambda r, n=1: dot(b_all[:, r * of : (r + n) * of], d_both, 0, 0).astype(BF16)

        def middle():
            two = by_b(1, 2)
            return two[:of], two[of:]

        by_gate, by_up = dp_scatter(by_b, middle, [ff, ff])
        dh = normed_back(db, h, dy)

        dhs = tp_gather(dh)

        def from_o(i, pieces, weights, tiles, outs, need):
            need(0, (0, nq), (0, d))
            for n in range(0, heads, 2):
                two = dot(pieces[0][i], weights[0][n * HEAD : (n + 2) * HEAD, :], 1, 1).astype(BF16)
                outs[0][n], outs[0][n + 1] = two[:, :HEAD], two[:, HEAD:]
                both = wide(two) * jnp.concatenate([wide(tiles[0][n]), wide(tiles[0][n + 1])], 1)
                outs[2][n : n + 1, :] = both[:, :HEAD].T.sum(0, keepdims=True)
                outs[2][n + 1 : n + 2, :] = both[:, HEAD:].T.sum(0, keepdims=True)
            outs[1][...] = pieces[0][i]

        kept = ()
        for r in (0, 2):
            kept = fused(from_o, 2, t * d * nq, [dhs[r : r + 2]], [by_place(w_o)], [(o, *by_head(r))],
                         [by_heads(r), whole(d, r), ((heads, t), F32, (heads, N), lambda i, r=r: (0, i + r))], kept)
        d_o, dh_all, delta = kept
        dw_o = lax.dot_general(o, dh_all, (((1,), (0,)), ((), ())), preferred_element_type=F32).astype(BF16).reshape(nq, d)
        by_o, = dp_scatter_by(2, lambda r: pick(dw_o, r, wo.shape[0]), [d])
        dq, dk, dv = attend_back(q, k, v, d_o, lse, delta, me)

        def to_a(i, pieces, weights, tiles, outs, need):
            cos, sin = tiles[3][...], tiles[4][...]
            back = lambda t: (wide(t) * cos - pltpu.roll(wide(t), half, 1) * sin).astype(BF16)
            one = jnp.concatenate([*(back(tiles[0][n]) for n in range(heads)), back(tiles[1][...]), tiles[2][...]], 1)
            outs[2][...] = one

            def into(out):
                def some(at):
                    need(0, (at, at + C), (0, width))
                    out[:, pl.ds(place_of(at, d // 4), C)] = dot(outs[2][...], weights[0][pl.ds(at, C), :], 1, 1).astype(BF16)

                chunks(d, some)

            each(i, outs[:2], into)

        far, near = (fused(to_a, 2, t * d * width, [], [by_distance(w_qkv)],
                           [(dq, *by_head(r)), (dk, (N, HEAD), tokens(r)), (dv, (N, HEAD), tokens(r)), (cos, (N, HEAD), tokens(r)), (sin, (N, HEAD), tokens(r))],
                           [*pair, ((t // 2, width), BF16, (N, width), tokens())]) for r in (2, 0))
        da = tp_scatter(far[:2], near[:2])
        d_qkv = jnp.concatenate([near[2], far[2]], 0)
        by_a = lambda r, n=1: dot(a_all[:, r * of : (r + n) * of], d_qkv, 0, 0).astype(BF16)

        def middle_a():
            two = by_a(1, 2)
            return two[:of], two[of:]

        by_q, by_k, by_v = dp_scatter(by_a, middle_a, [nq, nk, nk])
        dx = normed_back(da, x, dh)
        return dx[None], by_q, by_k, by_v, by_o, by_gate, by_up, by_down

    states, by_columns, by_rows = P("dp", "tp", None), P("dp", "tp"), P(("tp", "dp"), None)
    weights = (by_columns, by_columns, by_columns, by_rows, by_columns, by_columns, by_rows)
    return jax.shard_map(step, mesh=mesh, in_specs=(states, states, *weights), out_specs=(states, *weights), check_vma=False)
```
